512 devices in a mesh: prow: 16 (over z_hi, y, core), pcol: 32 (over z_lo, x).
Axes of the slice: x: 4, y: 4, z: 16 (z_hi: 2, z_lo: 8; z = z_hi * 8 + z_lo), core: 2. Of those that a mesh axis runs over, the one named last changes fastest.
Arguments:
- inverse_tiles: float32 [32, 16384, 512], P('prow', 'pcol'), may hold values from -0.36 to 0.36
- tile_rows: int32 [32, 32], P('prow', 'pcol'), may hold values from -1 to 1, as said below
- panel: float32 [16384, 1024], P(('prow', 'pcol')), may hold values from -0.6 to 0.6
- pivot_base: float32 [1024, 512], P('pcol'), may hold values from -6 to 6
Outputs:
- panel_inverse: float32 [16384, 1024], P(('prow', 'pcol'))
- pivot_inverse: float32 [1024, 512], P('pcol')
The draws below stay inside these ranges and needn't reach their ends.
Inputs may be any that keep to these rules, and one draw needn't show every extreme that they name: `tile_rows`: on each device the entries name distinct row tiles first and -1 after; the device at prow 0 and pcol 0 lists 2.
All inputs are finite; a program needn't handle non-finite values.
Results may differ from the reference program's by a relative error of at most 0.0003.
Values sent between devices are 32-bit elements; how exact they have to be, the bound alone decides.
No kernel may reach another device: no remote copies, remote signals or barrier semaphores. Data moves between devices by JAX's collectives and lax.ppermute only.
A program may use at most 64 MiB of HBM per device.

```python
import jax
import jax.numpy as jnp
from jax import lax

BS = 512
SUPER = 2
SLOTS = 2
RTILES = 2
ROWS = 16384
N_PROW = 16
N_PCOL = 32


def draw_tile_rows(key, part):
    base = jax.random.fold_in(key, 11)
    key_count, key_first = jax.random.split(base, 2)
    counts = jax.random.randint(key_count, (N_PROW, N_PCOL), 0, 3)
    counts = counts.at[0, 0].set(2)
    first = jax.random.randint(key_first, (N_PROW, N_PCOL), 0, 2)
    slot_zero = jnp.where(counts >= 1, first, -1)
    slot_one = jnp.where(counts == 2, 1 - first, -1)
    return jnp.stack([slot_zero, slot_one], axis=1).reshape(N_PROW * 2, N_PCOL).astype(jnp.int32)


def block_scale(key, dims, cuts, low, top_value):
    factor_of = 1.0
    for position, blocks in cuts:
        steps = jax.random.uniform(jax.random.fold_in(jax.random.fold_in(key, 6), position), (blocks,), jnp.float32, low / len(cuts), top_value / len(cuts))
        factor_of = factor_of * jnp.repeat(jnp.exp(steps), dims[position] // blocks).reshape((-1,) + (1,) * (len(dims) - 1 - position))
    return factor_of


def bell_draw(key, extent, scale, reach, shards=(), kind=jnp.bfloat16):
    result = jax.random.normal(key, extent, jnp.float32) * scale
    if len(shards) > 0:
        result = block_scale(key, extent, shards, -0.22, 0.18) * result
    return jnp.clip(result, min=-reach, max=reach).astype(kind)


def setup_inputs(seed: int = 0) -> dict:
    key_list = jax.random.split(jax.random.key(seed), 5)
    inverse_tiles = bell_draw(key_list[0], (SLOTS * N_PROW, BS * N_PCOL, BS), 0.06, 0.36, ((0, 16), (1, 32)), jnp.float32)
    tile_rows = draw_tile_rows(jax.random.fold_in(key_list[4], 71), 0)
    panel = bell_draw(key_list[2], (ROWS, SUPER * BS), 0.1, 0.6, ((0, 512),), jnp.float32)
    pivot_base = bell_draw(key_list[3], (SUPER * BS, BS), 1.0, 6.0, ((0, 32),), jnp.float32)
    return dict(inverse_tiles=inverse_tiles, tile_rows=tile_rows, panel=panel, pivot_base=pivot_base)


def reference(inverse_tiles, tile_rows, panel, pivot_base):
    grid_rows = N_PROW
    grid_cols = N_PCOL
    width = panel.shape[1]
    share = (2 * BS) // grid_cols
    columns = panel.reshape(grid_rows, grid_cols, share, width).transpose(1, 0, 2, 3).reshape(grid_cols, grid_rows * share, width)
    tiles = inverse_tiles.reshape(grid_rows, SLOTS, grid_cols, BS, BS)
    codes = tile_rows.reshape(grid_rows, SLOTS, grid_cols)
    levels = jnp.arange(RTILES, dtype=jnp.int32)

    def block_row(inputs):
        row_tiles, row_codes = inputs
        products = jnp.einsum("sqab,qbw->sqaw", row_tiles, columns, precision=lax.Precision.HIGHEST)
        placing = (row_codes[:, :, None] == levels[None, None, :]).astype(jnp.float32)
        return jnp.einsum("sqr,sqaw->raw", placing, products, precision=lax.Precision.HIGHEST)

    trailing_product = lax.map(block_row, (tiles, codes)).reshape(panel.shape[0], width)
    panel_inverse = -trailing_product
    upper = panel.reshape(-1, SUPER, BS)
    lower = trailing_product.reshape(-1, SUPER, BS)
    update = jnp.einsum("rka,rkb->kab", upper, lower, precision=lax.Precision.HIGHEST)
    pivot_inverse = pivot_base + update.reshape(SUPER * BS, BS)
    return panel_inverse, pivot_inverse
```

```python
import jax
import jax.numpy as jnp
from jax import lax
from jax.sharding import Mesh
from jax.sharding import PartitionSpec as P

HIGH = lax.Precision.HIGH
PROW = ("zh", "y", "c")
PCOL = ("zl", "x")


def shift(x, axis, by):
    n = lax.axis_size(axis)
    return lax.ppermute(x, axis, [(i, (i + by) % n) for i in range(n)])


def swap(x, axis, bit):
    n = lax.axis_size(axis)
    return lax.ppermute(x, axis, [(i, i ^ bit) for i in range(n)])


def ordered(mine, other, bit, axis):
    low = bit == 0
    return jnp.stack([jnp.where(low, mine, other), jnp.where(low, other, mine)], axis)


def pick(x, index, axis):
    return lax.dynamic_index_in_dim(x, index, axis, keepdims=False)


def dot(a, b, dims=(((1,), (0,)), ((), ()))):
    return lax.dot_general(a, b, dims, precision=HIGH, preferred_element_type=jnp.float32)


def gathered_column(panel):
    c = lax.axis_index("c")
    zh = lax.axis_index("zh")
    far = swap(panel, "zh", 1)
    halves = []
    for rows in (panel, far):
        mine = lax.all_gather(rows, "y", axis=0)
        halves.append(ordered(mine, swap(mine, "c", 1), c, 1))
    return ordered(halves[0], halves[1], zh, 0)


def gathered_over_zl(rows):
    zl = lax.axis_index("zl")
    rows = rows[None]
    for bit in (4, 2, 1):
        other = swap(rows, "zl", bit)
        rows = ordered(rows, other, zl & bit, 1 if bit != 4 else 0)
        rows = rows.reshape(-1, *rows.shape[2:])
    return rows


def products(inverse_tiles, codes, column):
    x = lax.axis_index("x")
    slots, block = inverse_tiles.shape[:2]
    tiles = inverse_tiles.reshape(slots, 4, 4, block // 16, block)
    column = column.reshape(block, -1)
    out = {}
    for d in (2, 1, 3, 0):
        part = pick(tiles, (x + d) % 4, 2)
        for i in range(2):
            left = jnp.where(codes[0] == i, part[0], jnp.where(codes[1] == i, part[1], 0.0))
            out[d, i] = dot(left.reshape(block // 4, block), column)
    return out


def reduced_over_x(t):
    up_a = shift(t[2, 0], "x", 1)
    down_a = shift(t[2, 1], "x", -1)
    up_b = shift(t[1, 1], "x", 1)
    down_b = shift(t[3, 0], "x", -1)
    up_c = shift(t[1, 0] + up_a, "x", 1)
    down_c = shift(t[3, 1] + down_a, "x", -1)
    return jnp.stack([t[0, 0] + down_b + up_c, t[0, 1] + up_b + down_c])


def reduced_over_zl(t):
    zl = lax.axis_index("zl")
    for bit, axis in ((1, 2), (2, 1), (4, 0)):
        mine = (zl // bit) % 2
        t = pick(t, mine, axis) + swap(pick(t, 1 - mine, axis), "zl", bit)
    return t


def local(inverse_tiles, tile_rows, panel, pivot_base):
    share, width = panel.shape
    block = inverse_tiles.shape[1]
    half = block // 2
    c = lax.axis_index("c")
    codes = tile_rows[:, 0]
    column = gathered_column(panel)
    upper = gathered_over_zl(panel)
    t = reduced_over_x(products(inverse_tiles, codes, column))
    trailing = reduced_over_zl(t.reshape(2, 2, 2, share, width))

    u = upper.reshape(8 * share, 2, block)
    v = t.reshape(8 * share, 2, 2, half)
    pair = (((0,), (0,)), ((1,), (1,)))
    away = dot(u, pick(v, 1 - c, 2), pair)
    home = dot(u, pick(v, c, 2), pair)
    w = home + swap(away, "c", 1)
    w = w.reshape(8, 4, 4, 8, half).transpose(2, 1, 0, 3, 4)
    w = w.reshape(16, 8, 8, half)
    w = lax.all_to_all(w, ("y", "x"), 0, 0, tiled=True).sum(axis=0)
    w = lax.all_to_all(w, "zl", 0, 0, tiled=True).sum(axis=0)
    w = lax.all_gather(w, PROW, axis=0).reshape(2, 4, 2, 8, half).sum(axis=0)
    w = w.transpose(0, 2, 1, 3).reshape(share, block)
    return (-trailing, pivot_base + w)


def solution(mesh):
    finer = Mesh(mesh.devices.reshape(2, 4, 2, 8, 4), PROW + PCOL)
    placed = (P(PROW, PCOL, None), P(PROW, PCOL), P(PROW + PCOL, None), P(PCOL, None))
    return jax.shard_map(
        local,
        mesh=finer,
        in_specs=placed,
        out_specs=(P(PROW + PCOL, None), P(PCOL, None)),
        check_vma=False,
    )
```

```python
import jax
import jax.numpy as jnp
from jax import lax
from jax.sharding import Mesh
from jax.sharding import PartitionSpec as P

HIGH = lax.Precision.HIGH
PROW = ("zh", "y", "c")
PCOL = ("zl", "x")


def shift(x, axis, by):
    n = lax.axis_size(axis)
    return lax.ppermute(x, axis, [(i, (i + by) % n) for i in range(n)])


def swap(x, axis, bit):
    n = lax.axis_size(axis)
    return lax.ppermute(x, axis, [(i, i ^ bit) for i in range(n)])


def spread(x, axes):
    copies = jnp.broadcast_to(x, (lax.axis_size(axes), *x.shape))
    return lax.all_to_all(copies, axes, 0, 0, tiled=True)


def ordered(mine, other, bit, axis):
    low = bit == 0
    return jnp.stack([jnp.where(low, mine, other), jnp.where(low, other, mine)], axis)


def pick(x, index, axis):
    return lax.dynamic_index_in_dim(x, index, axis, keepdims=False)


def dot(a, b):
    return jnp.dot(a, b, precision=HIGH, preferred_element_type=jnp.float32)


def gathered_column(panel):
    c = lax.axis_index("c")
    zh = lax.axis_index("zh")
    far = swap(panel, "zh", 1)
    near = spread(panel, "y")
    far = spread(far, "y")
    near = ordered(near, swap(near, "c", 1), c, 1)
    far = ordered(far, swap(far, "c", 1), c, 1)
    return ordered(near, far, zh, 0)


def gathered_over_zl(rows):
    zl = lax.axis_index("zl")
    rows = rows[None]
    for bit in (4, 2, 1):
        other = swap(rows, "zl", bit)
        rows = ordered(rows, other, zl & bit, 1 if bit != 4 else 0)
        rows = rows.reshape(-1, *rows.shape[2:])
    return rows


def reduced_products(inverse_tiles, codes, column):
    x = lax.axis_index("x")
    slots, block = inverse_tiles.shape[:2]
    tiles = inverse_tiles.reshape(slots, 4, 4, block // 16, block)
    column = column.reshape(block, -1)

    def product(d, i):
        part = pick(tiles, (x + d) % 4, 2)
        left = jnp.where(codes[0] == i, part[0], jnp.where(codes[1] == i, part[1], 0.0))
        return dot(left.reshape(block // 4, block), column)

    up_a = shift(product(2, 0), "x", 1)
    down_a = shift(product(2, 1), "x", -1)
    up_b = shift(product(1, 1), "x", 1)
    down_b = shift(product(3, 0), "x", -1)
    up_c = shift(product(1, 0) + up_a, "x", 1)
    down_c = shift(product(3, 1) + down_a, "x", -1)
    return product(0, 0) + down_b + up_c, product(0, 1) + up_b + down_c


def reduced_over_zl(t):
    zl = lax.axis_index("zl")
    for bit, axis in ((1, 2), (2, 1), (4, 0)):
        mine = (zl // bit) % 2
        t = pick(t, mine, axis) + swap(pick(t, 1 - mine, axis), "zl", bit)
    return t


def local(inverse_tiles, tile_rows, panel, pivot_base):
    share, width = panel.shape
    block = inverse_tiles.shape[1]
    half = block // 2
    c = lax.axis_index("c")
    codes = tile_rows[:, 0]
    column = gathered_column(panel)
    u = gathered_over_zl(panel).reshape(8 * share, width).T
    t = jnp.concatenate(reduced_products(inverse_tiles, codes, column))
    trailing = reduced_over_zl(t.reshape(2, 2, 2, share, width))

    def pivot(side):
        parts = []
        for j in range(2):
            v = lax.dynamic_slice_in_dim(t[:, j * block : (j + 1) * block], side * half, half, 1)
            parts.append(dot(u[j * block : (j + 1) * block], v))
        return jnp.stack(parts)

    away = swap(pivot(1 - c), "c", 1)
    w = pivot(c) + away
    w = w.reshape(8, 4, 4, 8, half).transpose(2, 1, 0, 3, 4)
    w = w.reshape(16, 8, 8, half)
    w = lax.all_to_all(w, ("y", "x"), 0, 0, tiled=True).sum(axis=0)
    w = jnp.concatenate([w, w])
    w = lax.all_to_all(w, ("zh", "zl"), 0, 0, tiled=True).sum(axis=0)
    w = spread(w, ("y", "c"))
    w = w.reshape(4, 2, 8, half).transpose(0, 2, 1, 3).reshape(share, block)
    return (-trailing, pivot_base + w)


def solution(mesh):
    finer = Mesh(mesh.devices.reshape(2, 4, 2, 8, 4), PROW + PCOL)
    placed = (P(PROW, PCOL, None), P(PROW, PCOL), P(PROW + PCOL, None), P(PCOL, None))

    return jax.shard_map(
        local,
        mesh=finer,
        in_specs=placed,
        out_specs=(P(PROW + PCOL, None), P(PCOL, None)),
        check_vma=False,
    )
```

```python
import jax
import jax.numpy as jnp
from jax import lax
from jax.sharding import Mesh
from jax.sharding import PartitionSpec as P

HIGH = lax.Precision.HIGH
PROW = ("zh", "y", "c")
PCOL = ("zl", "x")


def shift(x, axis, by):
    n = lax.axis_size(axis)
    return lax.ppermute(x, axis, [(i, (i + by) % n) for i in range(n)])


def swap(x, axis, bit):
    n = lax.axis_size(axis)
    return lax.ppermute(x, axis, [(i, i ^ bit) for i in range(n)])


def spread(x, axes):
    copies = jnp.broadcast_to(x, (lax.axis_size(axes), *x.shape))
    return lax.all_to_all(copies, axes, 0, 0, tiled=True)


def ordered(mine, other, bit, axis):
    low = bit == 0
    return jnp.stack([jnp.where(low, mine, other), jnp.where(low, other, mine)], axis)


def pick(x, index, axis):
    return lax.dynamic_index_in_dim(x, index, axis, keepdims=False)


def dot(a, b):
    return jnp.dot(a, b, precision=HIGH, preferred_element_type=jnp.float32)


def gathered_column(panel):
    c = lax.axis_index("c")
    zh = lax.axis_index("zh")
    y = lax.axis_index("y")
    far = swap(panel, "zh", 1)
    got = [panel]
    for k in (1, 2, 3):
        got.append(shift(panel, "y", -k))
    near = []
    for i in range(4):
        away = (i - y) % 4
        near.append(jnp.where(away < 2, jnp.where(away < 1, got[0], got[1]), jnp.where(away < 3, got[2], got[3])))
    near = jnp.stack(near)
    far = spread(far, "y")
    near = ordered(near, swap(near, "c", 1), c, 1)
    far = ordered(far, swap(far, "c", 1), c, 1)
    return ordered(near, far, zh, 0)


def gathered_over_zl(rows):
    zl = lax.axis_index("zl")
    rows = rows[None]
    for bit in (4, 2, 1):
        other = swap(rows, "zl", bit)
        rows = ordered(rows, other, zl & bit, 1 if bit != 4 else 0)
        rows = rows.reshape(-1, *rows.shape[2:])
    return rows


def reduced_over_zl(t):
    zl = lax.axis_index("zl")
    for bit, axis in ((1, 2), (2, 1), (4, 0)):
        mine = (zl // bit) % 2
        t = pick(t, mine, axis) + swap(pick(t, 1 - mine, axis), "zl", bit)
    return t


def reduced_products(inverse_tiles, codes, column):
    x = lax.axis_index("x")
    slots, block = inverse_tiles.shape[:2]
    tiles = inverse_tiles.reshape(slots, 4, 4, block // 16, block)
    column = column.reshape(block, -1)

    def product(d, i):
        part = pick(tiles, (x + d) % 4, 2)
        left = jnp.where(codes[0] == i, part[0], jnp.where(codes[1] == i, part[1], 0.0))
        return dot(left.reshape(block // 4, block), column)

    up_a = shift(product(2, 0), "x", 1)
    down_a = shift(product(2, 1), "x", -1)
    up_b = shift(product(1, 1), "x", 1)
    down_b = shift(product(3, 0), "x", -1)
    rest = [product(*di) for di in ((1, 0), (3, 1), (0, 0), (0, 1))]
    rest = lax.optimization_barrier(rest)
    up_c = shift(rest[0] + up_a, "x", 1)
    down_c = shift(rest[1] + down_a, "x", -1)
    return rest[2] + down_b + up_c, rest[3] + up_b + down_c


def local(inverse_tiles, tile_rows, panel, pivot_base):
    share, width = panel.shape
    block = inverse_tiles.shape[1]
    half = block // 2
    c = lax.axis_index("c")
    codes = tile_rows[:, 0]
    column = gathered_column(panel)
    u = gathered_over_zl(panel).reshape(8 * share, width).T
    u = u.reshape(2, 4, 4, 4, 8, 8 * share).transpose(0, 3, 2, 1, 4, 5)
    u = lax.optimization_barrier(u.reshape(2, block, 8 * share))
    other_u = swap(u, "c", 1)
    t = jnp.concatenate(reduced_products(inverse_tiles, codes, column))
    trailing = reduced_over_zl(t.reshape(2, 2, 2, share, width))

    def side(which):
        first = which * half
        cut = [lax.dynamic_slice_in_dim(t, first + j * block, half, 1) for j in range(2)]
        return jnp.stack(cut)

    other_t = swap(side(1 - c), "c", 1)
    mine = side(c)
    own = lax.optimization_barrier([dot(u[j], mine[j]) for j in range(2)])
    w = [own[j] + dot(other_u[j], other_t[j]) for j in range(2)]
    w = jnp.concatenate([x.reshape(16, 4, 8, half) for x in w], axis=1)
    w = lax.all_to_all(w, ("y", "x"), 0, 0, tiled=True).sum(axis=0)
    w = jnp.concatenate([w, w])
    w = lax.all_to_all(w, ("zh", "zl"), 0, 0, tiled=True).sum(axis=0)
    w = spread(w, ("y", "c"))
    w = w.reshape(4, 2, 8, half).transpose(0, 2, 1, 3).reshape(share, block)
    return (-trailing, pivot_base + w)


def solution(mesh):
    finer = Mesh(mesh.devices.reshape(2, 4, 2, 8, 4), PROW + PCOL)
    placed = (P(PROW, PCOL, None), P(PROW, PCOL), P(PROW + PCOL, None), P(PCOL, None))

    return jax.shard_map(
        local,
        mesh=finer,
        in_specs=placed,
        out_specs=(P(PROW + PCOL, None), P(PCOL, None)),
        check_vma=False,
    )
```

```python
import jax
import jax.numpy as jnp
from jax import lax
from jax.sharding import Mesh
from jax.sharding import PartitionSpec as P

HIGH = lax.Precision.HIGH
PROW = ("zh", "y", "c")
PCOL = ("zl", "x")


def shift(x, axis, by):
    n = lax.axis_size(axis)
    return lax.ppermute(x, axis, [(i, (i + by) % n) for i in range(n)])


def swap(x, axis, bit):
    n = lax.axis_size(axis)
    return lax.ppermute(x, axis, [(i, i ^ bit) for i in range(n)])


def spread(x, axes):
    copies = jnp.broadcast_to(x, (lax.axis_size(axes), *x.shape))
    return lax.all_to_all(copies, axes, 0, 0, tiled=True)


def ordered(mine, other, bit, axis):
    low = bit == 0
    return jnp.stack([jnp.where(low, mine, other), jnp.where(low, other, mine)], axis)


def pick(x, index, axis):
    return lax.dynamic_index_in_dim(x, index, axis, keepdims=False)


def dot(a, b):
    return jnp.dot(a, b, precision=HIGH, preferred_element_type=jnp.float32)


def gathered_column(panel):
    c = lax.axis_index("c")
    zh = lax.axis_index("zh")
    y = lax.axis_index("y")
    far = swap(panel, "zh", 1)
    got = [panel]
    for k in (1, 2, 3):
        got.append(shift(panel, "y", -k))
    near = []
    for i in range(4):
        away = (i - y) % 4
        near.append(jnp.where(away < 2, jnp.where(away < 1, got[0], got[1]), jnp.where(away < 3, got[2], got[3])))
    near = jnp.stack(near)
    far = spread(far, "y")
    near = ordered(near, swap(near, "c", 1), c, 1)
    far = ordered(far, swap(far, "c", 1), c, 1)
    return ordered(near, far, zh, 0)


def gathered_over_zl(rows):
    zl = lax.axis_index("zl")
    rows = rows[None]
    for bit in (4, 2, 1):
        other = swap(rows, "zl", bit)
        rows = ordered(rows, other, zl & bit, 1 if bit != 4 else 0)
        rows = rows.reshape(-1, *rows.shape[2:])
    return rows


def reduced_over_zl(halves):
    zl = lax.axis_index("zl")
    low, mid, high = zl % 2, (zl // 2) % 2, zl // 4
    rows = []
    for t in halves:
        t = t.reshape(2, 2, -1, t.shape[-1])
        rows.append(pick(t, low, 1) + swap(pick(t, 1 - low, 1), "zl", 1))
    kept = [pick(t, mid, 0) for t in rows]
    sent = jnp.stack([pick(t, 1 - mid, 0) for t in rows])
    sent = swap(sent, "zl", 2)
    rows = [kept[i] + sent[i] for i in range(2)]
    first = high == 0
    sent = swap(jnp.where(first, rows[1], rows[0]), "zl", 4)
    return jnp.where(first, rows[0], rows[1]) + sent


def reduced_products(inverse_tiles, codes, column):
    x = lax.axis_index("x")
    slots, block = inverse_tiles.shape[:2]
    tiles = inverse_tiles.reshape(slots, 4, 4, block // 16, block)
    column = column.reshape(block, -1)

    def product(d, i):
        part = pick(tiles, (x + d) % 4, 2)
        left = jnp.where(codes[0] == i, part[0], jnp.where(codes[1] == i, part[1], 0.0))
        return dot(left.reshape(block // 4, block), column)

    up_a = shift(product(2, 0), "x", 1)
    down_a = shift(product(2, 1), "x", -1)
    up_b = shift(product(1, 1), "x", 1)
    down_b = shift(product(3, 0), "x", -1)
    rest = [product(*di) for di in ((1, 0), (3, 1), (0, 0), (0, 1))]
    rest = lax.optimization_barrier(rest)
    up_c = shift(rest[0] + up_a, "x", 1)
    down_c = shift(rest[1] + down_a, "x", -1)
    first = rest[2] + down_b + up_c
    return first, rest[3] + up_b + down_c


def local(inverse_tiles, tile_rows, panel, pivot_base):
    share, width = panel.shape
    block = inverse_tiles.shape[1]
    half = block // 2
    c = lax.axis_index("c")
    codes = tile_rows[:, 0]
    column = gathered_column(panel)
    u = gathered_over_zl(panel).reshape(8 * share, width).T
    u = u.reshape(2, 4, 4, 4, 8, 8 * share).transpose(0, 3, 2, 1, 4, 5)
    u = lax.optimization_barrier(u.reshape(2, block, 8 * share))
    other_u = swap(u, "c", 1)
    halves = reduced_products(inverse_tiles, codes, column)
    trailing = reduced_over_zl(halves)

    def side(t, which):
        first = which * half
        cut = [lax.dynamic_slice_in_dim(t, first + j * block, half, 1) for j in range(2)]
        return jnp.stack(cut)

    mine, other = [], []
    for t in halves:
        other.append(swap(side(t, 1 - c), "c", 1))
        mine.append(side(t, c))
    k = 4 * share
    own = [dot(u[j, :, :k], mine[0][j]) for j in range(2)]
    own = lax.optimization_barrier(own)
    own = [own[j] + dot(u[j, :, k:], mine[1][j]) for j in range(2)]
    own = lax.optimization_barrier(own)
    other = [jnp.concatenate([other[0][j], other[1][j]]) for j in range(2)]
    w = [own[j] + dot(other_u[j], other[j]) for j in range(2)]
    w = jnp.concatenate([x.reshape(16, 4, 8, half) for x in w], axis=1)
    w = lax.all_to_all(w, ("y", "x"), 0, 0, tiled=True).sum(axis=0)
    w = jnp.concatenate([w, w])
    w = lax.all_to_all(w, ("zh", "zl"), 0, 0, tiled=True).sum(axis=0)
    w = spread(w, ("y", "c"))
    w = w.reshape(4, 2, 8, half).transpose(0, 2, 1, 3).reshape(share, block)
    return (-trailing, pivot_base + w)


def solution(mesh):
    finer = Mesh(mesh.devices.reshape(2, 4, 2, 8, 4), PROW + PCOL)
    placed = (P(PROW, PCOL, None), P(PROW, PCOL), P(PROW + PCOL, None), P(PCOL, None))

    return jax.shard_map(
        local,
        mesh=finer,
        in_specs=placed,
        out_specs=(P(PROW + PCOL, None), P(PCOL, None)),
        check_vma=False,
    )
```

```python
import jax
import jax.numpy as jnp
from jax import lax
from jax.sharding import Mesh
from jax.sharding import PartitionSpec as P

HIGH = lax.Precision.HIGH
PROW = ("zh", "y", "c")
PCOL = ("zl", "x")


def shift(x, axis, by):
    n = lax.axis_size(axis)
    return lax.ppermute(x, axis, [(i, (i + by) % n) for i in range(n)])


def swap(x, axis, bit):
    n = lax.axis_size(axis)
    return lax.ppermute(x, axis, [(i, i ^ bit) for i in range(n)])


def spread(x, axes):
    copies = jnp.broadcast_to(x, (lax.axis_size(axes), *x.shape))
    return lax.all_to_all(copies, axes, 0, 0, tiled=True)


def ordered(mine, other, bit, axis):
    low = bit == 0
    return jnp.stack([jnp.where(low, mine, other), jnp.where(low, other, mine)], axis)


def pick(x, index, axis):
    return lax.dynamic_index_in_dim(x, index, axis, keepdims=False)


def dot(a, b):
    return jnp.dot(a, b, precision=HIGH, preferred_element_type=jnp.float32)


def pair(a, b):
    dims = (((2,), (1,)), ((0,), (0,)))
    return lax.dot_general(a, b, dims, precision=HIGH, preferred_element_type=jnp.float32)


def gathered_column(panel):
    c = lax.axis_index("c")
    zh = lax.axis_index("zh")
    y = lax.axis_index("y")
    far = swap(panel, "zh", 1)
    got = [panel]
    for k in (1, 2, 3):
        got.append(shift(panel, "y", -k))
    near = []
    for i in range(4):
        away = (i - y) % 4
        near.append(jnp.where(away < 2, jnp.where(away < 1, got[0], got[1]), jnp.where(away < 3, got[2], got[3])))
    near = jnp.stack(near)
    far = spread(far, "y")
    near = ordered(near, swap(near, "c", 1), c, 1)
    far = ordered(far, swap(far, "c", 1), c, 1)
    return ordered(near, far, zh, 0)


def gathered_over_zl(rows):
    zl = lax.axis_index("zl")
    rows = rows[None]
    for bit in (4, 2, 1):
        other = swap(rows, "zl", bit)
        rows = ordered(rows, other, zl & bit, 1 if bit != 4 else 0)
        rows = rows.reshape(-1, *rows.shape[2:])
    return rows


def reduced_over_zl(halves):
    zl = lax.axis_index("zl")
    low, mid, high = zl % 2, (zl // 2) % 2, zl // 4
    rows = []
    for t in halves:
        t = t.reshape(2, 2, -1, t.shape[-1])
        rows.append(pick(t, low, 1) + swap(pick(t, 1 - low, 1), "zl", 1))
    for i, t in enumerate(rows):
        rows[i] = pick(t, mid, 0) + swap(pick(t, 1 - mid, 0), "zl", 2)
    first = high == 0
    sent = swap(jnp.where(first, rows[1], rows[0]), "zl", 4)
    return jnp.where(first, rows[0], rows[1]) + sent


def reduced_products(inverse_tiles, codes, column):
    x = lax.axis_index("x")
    slots, block = inverse_tiles.shape[:2]
    tiles = inverse_tiles.reshape(slots, 4, 4, block // 16, block)
    column = column.reshape(block, -1)

    def product(d, i):
        part = pick(tiles, (x + d) % 4, 2)
        left = jnp.where(codes[0] == i, part[0], jnp.where(codes[1] == i, part[1], 0.0))
        return dot(left.reshape(block // 4, block), column)

    up_a = shift(product(2, 0), "x", 1)
    down_a = shift(product(2, 1), "x", -1)
    up_b = shift(product(1, 1), "x", 1)
    down_b = shift(product(3, 0), "x", -1)
    rest = lax.optimization_barrier([product(1, 0), product(3, 1)])
    up_c = shift(rest[0] + up_a, "x", 1)
    down_c = shift(rest[1] + down_a, "x", -1)
    first = product(0, 0) + down_b + up_c
    return first, product(0, 1) + up_b + down_c


def local(inverse_tiles, tile_rows, panel, pivot_base):
    share, width = panel.shape
    block = inverse_tiles.shape[1]
    half = block // 2
    c = lax.axis_index("c")
    codes = tile_rows[:, 0]
    column = gathered_column(panel)
    u = gathered_over_zl(panel).reshape(8 * share, width).T
    u = u.reshape(2, 4, 4, 4, 8, 8 * share).transpose(0, 3, 2, 1, 4, 5)
    u = lax.optimization_barrier(u.reshape(2, block, 8 * share))
    other_u = swap(u, "c", 1)
    halves = reduced_products(inverse_tiles, codes, column)
    trailing = reduced_over_zl(halves)

    def side(t, which):
        first = which * half
        cut = [lax.dynamic_slice_in_dim(t, first + j * block, half, 1) for j in range(2)]
        return jnp.stack(cut)

    mine, other = [], []
    for t in halves:
        other.append(swap(side(t, 1 - c), "c", 1))
        mine.append(side(t, c))
    k = 4 * share
    cuts = (slice(0, k), slice(k, 2 * k))
    own = pair(u[:, :, cuts[0]], mine[0])
    own = lax.optimization_barrier(own)
    own = own + pair(u[:, :, cuts[1]], mine[1])
    own = lax.optimization_barrier(own)
    for i in range(2):
        own = own + pair(other_u[:, :, cuts[i]], other[i])
    w = own.reshape(2, 16, 4, 8, half).transpose(1, 0, 2, 3, 4).reshape(16, 8, 8, half)
    w = lax.all_to_all(w, ("y", "x"), 0, 0, tiled=True).sum(axis=0)
    w = jnp.concatenate([w, w])
    w = lax.all_to_all(w, ("zh", "zl"), 0, 0, tiled=True).sum(axis=0)
    w = spread(w, ("y", "c"))
    w = w.reshape(4, 2, 8, half).transpose(0, 2, 1, 3).reshape(share, block)
    return (-trailing, pivot_base + w)


def solution(mesh):
    finer = Mesh(mesh.devices.reshape(2, 4, 2, 8, 4), PROW + PCOL)
    placed = (P(PROW, PCOL, None), P(PROW, PCOL), P(PROW + PCOL, None), P(PCOL, None))

    return jax.shard_map(
        local,
        mesh=finer,
        in_specs=placed,
        out_specs=(P(PROW + PCOL, None), P(PCOL, None)),
        check_vma=False,
    )
```

```python
import jax
import jax.numpy as jnp
from jax import lax
from jax.sharding import Mesh
from jax.sharding import PartitionSpec as P

HIGH = lax.Precision.HIGH
PROW = ("zh", "y", "c")
PCOL = ("zl", "x")


def shift(x, axis, by):
    n = lax.axis_size(axis)
    return lax.ppermute(x, axis, [(i, (i + by) % n) for i in range(n)])


def swap(x, axis, bit):
    n = lax.axis_size(axis)
    return lax.ppermute(x, axis, [(i, i ^ bit) for i in range(n)])


def spread(x, axes):
    copies = jnp.broadcast_to(x, (lax.axis_size(axes), *x.shape))
    return lax.all_to_all(copies, axes, 0, 0, tiled=True)


def ordered(mine, other, bit, axis):
    low = bit == 0
    return jnp.stack([jnp.where(low, mine, other), jnp.where(low, other, mine)], axis)


def pick(x, index, axis):
    return lax.dynamic_index_in_dim(x, index, axis, keepdims=False)


def dot(a, b):
    return jnp.dot(a, b, precision=HIGH, preferred_element_type=jnp.float32)


def gathered_column(panel):
    c = lax.axis_index("c")
    zh = lax.axis_index("zh")
    far = swap(panel, "zh", 1)
    both = jnp.concatenate([jnp.broadcast_to(r, (4, *r.shape)) for r in (panel, far)], axis=1)
    both = lax.all_to_all(both, "y", 0, 0, tiled=True).reshape(4, 2, *panel.shape)
    both = ordered(both, swap(both, "c", 1), c, 2)
    low = zh == 0
    return jnp.stack([jnp.where(low, both[:, 0], both[:, 1]), jnp.where(low, both[:, 1], both[:, 0])])


def gathered_over_zl(rows):
    zl = lax.axis_index("zl")
    rows = rows[None]
    for bit in (4, 2, 1):
        other = swap(rows, "zl", bit)
        rows = ordered(rows, other, zl & bit, 1 if bit != 4 else 0)
        rows = rows.reshape(-1, *rows.shape[2:])
    return rows


def reduced_over_zl(t):
    zl = lax.axis_index("zl")
    for bit, axis in ((1, 2), (2, 1), (4, 0)):
        mine = (zl // bit) % 2
        t = pick(t, mine, axis) + swap(pick(t, 1 - mine, axis), "zl", bit)
    return t


def reduced_products(inverse_tiles, codes, column):
    x = lax.axis_index("x")
    slots, block = inverse_tiles.shape[:2]
    tiles = inverse_tiles.reshape(slots, 4, 4, block // 16, block)
    column = column.reshape(block, -1)
    left = {}
    for d in range(4):
        part = pick(tiles, (x + d) % 4, 2)
        for i in range(2):
            rows = jnp.where(codes[0] == i, part[0], jnp.where(codes[1] == i, part[1], 0.0))
            left[d, i] = rows.reshape(block // 4, block)

    def product(d, i):
        return dot(left[d, i], column)

    up_a = shift(product(2, 0), "x", 1)
    down_a = shift(product(2, 1), "x", -1)
    up_b = shift(product(1, 1), "x", 1)
    down_b = shift(product(3, 0), "x", -1)
    rest = lax.optimization_barrier([product(1, 0), product(3, 1)])
    up_c = shift(rest[0] + up_a, "x", 1)
    down_c = shift(rest[1] + down_a, "x", -1)
    return product(0, 0) + down_b + up_c, product(0, 1) + up_b + down_c


def local(inverse_tiles, tile_rows, panel, pivot_base):
    share, width = panel.shape
    block = inverse_tiles.shape[1]
    half = block // 2
    c = lax.axis_index("c")
    codes = tile_rows[:, 0]
    column = gathered_column(panel)
    u = gathered_over_zl(panel).reshape(8 * share, width).T
    u = u.reshape(2, 4, 4, 4, 8, 8 * share).transpose(0, 3, 2, 1, 4, 5)
    u = lax.optimization_barrier(u.reshape(2, block, 8 * share))
    other_u = swap(u, "c", 1)
    t = jnp.concatenate(reduced_products(inverse_tiles, codes, column))
    trailing = reduced_over_zl(t.reshape(2, 2, 2, share, width))

    def side(which):
        first = which * half
        cut = [lax.dynamic_slice_in_dim(t, first + j * block, half, 1) for j in range(2)]
        return jnp.stack(cut)

    other_t = swap(side(1 - c), "c", 1)
    mine = side(c)
    own = lax.optimization_barrier([dot(u[j], mine[j]) for j in range(2)])
    w = [own[j] + dot(other_u[j], other_t[j]) for j in range(2)]
    w = jnp.concatenate([x.reshape(16, 4, 8, half) for x in w], axis=1)
    w = lax.all_to_all(w, ("y", "x"), 0, 0, tiled=True).sum(axis=0)
    w = lax.all_to_all(w, "zl", 0, 0, tiled=True).sum(axis=0)
    w = spread(w, PROW)
    w = w[:8] + w[8:]
    w = w.reshape(4, 2, 8, half).transpose(0, 2, 1, 3).reshape(share, block)
    return (-trailing, pivot_base + w)


def solution(mesh):
    finer = Mesh(mesh.devices.reshape(2, 4, 2, 8, 4), PROW + PCOL)
    placed = (P(PROW, PCOL, None), P(PROW, PCOL), P(PROW + PCOL, None), P(PCOL, None))

    return jax.shard_map(
        local,
        mesh=finer,
        in_specs=placed,
        out_specs=(P(PROW + PCOL, None), P(PCOL, None)),
        check_vma=False,
    )
```

```python
import jax
import jax.numpy as jnp
from jax import lax
from jax.sharding import Mesh
from jax.sharding import PartitionSpec as P

HIGH = lax.Precision.HIGH
PROW = ("zh", "y", "c")
PCOL = ("zl", "x")


def shift(x, axis, by):
    n = lax.axis_size(axis)
    return lax.ppermute(x, axis, [(i, (i + by) % n) for i in range(n)])


def swap(x, axis, bit):
    n = lax.axis_size(axis)
    return lax.ppermute(x, axis, [(i, i ^ bit) for i in range(n)])


def spread(x, axes):
    copies = jnp.broadcast_to(x, (lax.axis_size(axes), *x.shape))
    return lax.all_to_all(copies, axes, 0, 0, tiled=True)


def ordered(mine, other, bit, axis):
    low = bit == 0
    return jnp.stack([jnp.where(low, mine, other), jnp.where(low, other, mine)], axis)


def pick(x, index, axis):
    return lax.dynamic_index_in_dim(x, index, axis, keepdims=False)


def dot(a, b):
    return jnp.dot(a, b, precision=HIGH, preferred_element_type=jnp.float32)


def gathered_column(panel):
    c = lax.axis_index("c")
    zh = lax.axis_index("zh")
    far = swap(panel, "zh", 1)
    both = jnp.concatenate([jnp.broadcast_to(r, (4, *r.shape)) for r in (panel, far)], axis=1)
    both = lax.all_to_all(both, "y", 0, 0, tiled=True).reshape(4, 2, *panel.shape)
    both = ordered(both, swap(both, "c", 1), c, 2)
    low = zh == 0
    return jnp.stack([jnp.where(low, both[:, 0], both[:, 1]), jnp.where(low, both[:, 1], both[:, 0])])


def gathered_over_zl(rows):
    zl = lax.axis_index("zl")
    rows = rows[None]
    for bit in (4, 2, 1):
        other = swap(rows, "zl", bit)
        rows = ordered(rows, other, zl & bit, 1 if bit != 4 else 0)
        rows = rows.reshape(-1, *rows.shape[2:])
    return rows


def reduced_over_zl(t):
    zl = lax.axis_index("zl")
    low, mid, high = zl % 2, (zl // 2) % 2, zl // 4
    t = pick(t, low, 2) + swap(pick(t, 1 - low, 2), "zl", 1)

    def part(flip_high, flip_mid):
        first = (high ^ flip_high, mid ^ flip_mid, 0, 0)
        return lax.dynamic_slice(t, first, (1, 1, *t.shape[2:]))[0, 0]

    got = []
    for flips in ((1, 1), (1, 0), (0, 1)):
        bit = flips[0] * 4 + flips[1] * 2
        got.append(swap(part(*flips), "zl", bit))
    return part(0, 0) + got[0] + got[1] + got[2]


def reduced_products(inverse_tiles, codes, column):
    x = lax.axis_index("x")
    slots, block = inverse_tiles.shape[:2]
    tiles = inverse_tiles.reshape(slots, 4, 4, block // 16, block)
    column = column.reshape(block, -1)
    left = {}
    for d in range(4):
        part = pick(tiles, (x + d) % 4, 2)
        for i in range(2):
            rows = jnp.where(codes[0] == i, part[0], jnp.where(codes[1] == i, part[1], 0.0))
            left[d, i] = rows.reshape(block // 4, block)

    def product(d, i):
        return dot(left[d, i], column)

    up_a = shift(product(2, 0), "x", 1)
    down_a = shift(product(2, 1), "x", -1)
    up_b = shift(product(1, 1), "x", 1)
    down_b = shift(product(3, 0), "x", -1)
    rest = lax.optimization_barrier([product(1, 0), product(3, 1)])
    up_c = shift(rest[0] + up_a, "x", 1)
    down_c = shift(rest[1] + down_a, "x", -1)
    return product(0, 0) + down_b + up_c, product(0, 1) + up_b + down_c


def local(inverse_tiles, tile_rows, panel, pivot_base):
    share, width = panel.shape
    block = inverse_tiles.shape[1]
    half = block // 2
    c = lax.axis_index("c")
    codes = tile_rows[:, 0]
    column = gathered_column(panel)
    u = gathered_over_zl(panel).reshape(8 * share, width).T
    u = u.reshape(2, 4, 4, 4, 8, 8 * share).transpose(0, 3, 2, 1, 4, 5)
    u = lax.optimization_barrier(u.reshape(2, block, 8 * share))
    other_u = swap(u, "c", 1)
    t = jnp.concatenate(reduced_products(inverse_tiles, codes, column))
    trailing = reduced_over_zl(t.reshape(2, 2, 2, share, width))

    def side(which):
        first = which * half
        cut = [lax.dynamic_slice_in_dim(t, first + j * block, half, 1) for j in range(2)]
        return jnp.stack(cut)

    other_t = swap(side(1 - c), "c", 1)
    mine = side(c)
    own = lax.optimization_barrier([dot(u[j], mine[j]) for j in range(2)])
    w = [own[j] + dot(other_u[j], other_t[j]) for j in range(2)]
    w = jnp.concatenate([x.reshape(16, 4, 8, half) for x in w], axis=1)
    w = lax.all_to_all(w, ("y", "x"), 0, 0, tiled=True).sum(axis=0)
    w = jnp.concatenate([w, w])
    w = lax.all_to_all(w, ("zh", "zl"), 0, 0, tiled=True).sum(axis=0)
    w = spread(w, ("y", "c"))
    w = w.reshape(4, 2, 8, half).transpose(0, 2, 1, 3).reshape(share, block)
    return (-trailing, pivot_base + w)


def solution(mesh):
    finer = Mesh(mesh.devices.reshape(2, 4, 2, 8, 4), PROW + PCOL)
    placed = (P(PROW, PCOL, None), P(PROW, PCOL), P(PROW + PCOL, None), P(PCOL, None))

    return jax.shard_map(
        local,
        mesh=finer,
        in_specs=placed,
        out_specs=(P(PROW + PCOL, None), P(PCOL, None)),
        check_vma=False,
    )
```

```python
import jax
import jax.numpy as jnp
from jax import lax
from jax.sharding import Mesh
from jax.sharding import PartitionSpec as P

HIGH = lax.Precision.HIGH
PROW = ("zh", "y", "c")
PCOL = ("zl", "x")


def shift(x, axis, by):
    n = lax.axis_size(axis)
    return lax.ppermute(x, axis, [(i, (i + by) % n) for i in range(n)])


def swap(x, axis, bit):
    n = lax.axis_size(axis)
    return lax.ppermute(x, axis, [(i, i ^ bit) for i in range(n)])


def spread(x, axes):
    copies = jnp.broadcast_to(x, (lax.axis_size(axes), *x.shape))
    return lax.all_to_all(copies, axes, 0, 0, tiled=True)


def ordered(mine, other, bit, axis):
    low = bit == 0
    return jnp.stack([jnp.where(low, mine, other), jnp.where(low, other, mine)], axis)


def pick(x, index, axis):
    return lax.dynamic_index_in_dim(x, index, axis, keepdims=False)


def dot(a, b):
    return jnp.dot(a, b, precision=HIGH, preferred_element_type=jnp.float32)


def gathered_column(panel):
    c = lax.axis_index("c")
    zh = lax.axis_index("zh")
    share, width = panel.shape
    part = width // 4

    def columns(which):
        first = which * part
        cuts = [lax.dynamic_slice_in_dim(panel, first + j * 2 * part, part, 1) for j in range(2)]
        return jnp.concatenate(cuts, axis=1)

    near = ordered(columns(c), swap(columns(1 - c), "c", 1), c, 0)
    near = near.reshape(2 * share, width // 2)
    far = swap(near, "zh", 1)
    both = jnp.concatenate([jnp.broadcast_to(r, (4, *r.shape)) for r in (near, far)], axis=1)
    both = lax.all_to_all(both, "y", 0, 0, tiled=True).reshape(4, 2, *near.shape)
    low = zh == 0
    return jnp.stack([jnp.where(low, both[:, 0], both[:, 1]), jnp.where(low, both[:, 1], both[:, 0])])


def gathered_over_zl(rows):
    zl = lax.axis_index("zl")
    rows = rows[None]
    for bit in (4, 2, 1):
        other = swap(rows, "zl", bit)
        rows = ordered(rows, other, zl & bit, 1 if bit != 4 else 0)
        rows = rows.reshape(-1, *rows.shape[2:])
    return rows


def reduced_over_zl(halves):
    zl = lax.axis_index("zl")
    low, mid, high = zl % 2, (zl // 2) % 2, zl // 4
    rows = []
    for t in halves:
        rows.append(pick(t, low, 2) + swap(pick(t, 1 - low, 2), "zl", 1))

    def part(flip_high, flip_mid):
        first = (high ^ flip_high, mid ^ flip_mid, 0, 0)
        return jnp.stack([lax.dynamic_slice(t, first, (1, 1, *t.shape[2:]))[0, 0] for t in rows])

    got = []
    for flips in ((0, 1), (1, 0), (1, 1)):
        bit = flips[0] * 4 + flips[1] * 2
        got.append(swap(part(*flips), "zl", bit))
    return part(0, 0) + got[0] + got[1] + got[2]


def reduced_products(inverse_tiles, codes, column):
    x = lax.axis_index("x")
    block = inverse_tiles.shape[1]
    column = column.reshape(block, -1)
    first, second = inverse_tiles
    tiles = [
        jnp.where(codes[0] == i, first, jnp.where(codes[1] == i, second, 0.0)) for i in range(2)
    ]
    tiles = lax.optimization_barrier(jnp.stack(tiles))
    tiles = (tiles, swap(tiles, "c", 1))
    left = {}
    for r in range(2):
        rows = tiles[r].reshape(2, 4, 4, block // 16, block)
        rows = [pick(rows, (x + d) % 4, 2).reshape(block // 2, block) for d in range(4)]
        for d, cut in enumerate(lax.optimization_barrier(rows)):
            left[d, r] = cut

    def product(d, r):
        return dot(left[d, r], column)

    up_a = shift(product(2, 0), "x", 1)
    down_a = shift(product(2, 1), "x", -1)
    up_b = shift(product(1, 1), "x", 1)
    down_b = shift(product(3, 0), "x", -1)
    rest = lax.optimization_barrier([product(1, 0), product(3, 1)])
    up_c = shift(rest[0] + up_a, "x", 1)
    down_c = shift(rest[1] + down_a, "x", -1)
    first = product(0, 0) + down_b + up_c
    return first, product(0, 1) + up_b + down_c


def local(inverse_tiles, tile_rows, panel, pivot_base):
    share, width = panel.shape
    block = inverse_tiles.shape[1]
    half = block // 2
    c = lax.axis_index("c")
    codes = tile_rows[:, 0]
    column = gathered_column(panel)
    u = gathered_over_zl(panel).reshape(8 * share, width).T
    u = u.reshape(2, 4, 4, 4, 8, 8 * share).transpose(0, 3, 2, 1, 4, 5)
    u = lax.optimization_barrier(u.reshape(2, block, 8 * share))
    other_u = swap(u, "c", 1)
    t = reduced_products(inverse_tiles, codes, column)
    trailing = reduced_over_zl([x.reshape(2, 2, 2, share, block) for x in t])
    other = swap(trailing[1], "c", 1)
    low, high = ordered(trailing[0], other, c, 0)
    trailing = [x[:, j * half : (j + 1) * half] for j in range(2) for x in (low, high)]
    trailing = jnp.concatenate(trailing, axis=1)

    parts = [[t[r][:, j * half : (j + 1) * half] for j in range(2)] for r in range(2)]
    own = lax.optimization_barrier([dot(u[j], parts[0][j]) for j in range(2)])
    w = [own[j] + dot(other_u[j], parts[1][j]) for j in range(2)]
    w = jnp.concatenate([x.reshape(16, 4, 8, half) for x in w], axis=1)
    w = lax.all_to_all(w, ("y", "x"), 0, 0, tiled=True).sum(axis=0)
    w = jnp.concatenate([w, w])
    w = lax.all_to_all(w, ("zh", "zl"), 0, 0, tiled=True).sum(axis=0)
    w = spread(w, ("y", "c"))
    w = w.reshape(4, 2, 8, half).transpose(0, 2, 1, 3).reshape(share, block)
    return (-trailing, pivot_base + w)


def solution(mesh):
    finer = Mesh(mesh.devices.reshape(2, 4, 2, 8, 4), PROW + PCOL)
    placed = (P(PROW, PCOL, None), P(PROW, PCOL), P(PROW + PCOL, None), P(PCOL, None))

    return jax.shard_map(
        local,
        mesh=finer,
        in_specs=placed,
        out_specs=(P(PROW + PCOL, None), P(PCOL, None)),
        check_vma=False,
    )
```

```python
import jax
import jax.numpy as jnp
from jax import lax
from jax.sharding import Mesh
from jax.sharding import PartitionSpec as P

HIGH = lax.Precision.HIGH
PROW = ("zh", "y", "c")
PCOL = ("zl", "x")


def shift(x, axis, by):
    n = lax.axis_size(axis)
    return lax.ppermute(x, axis, [(i, (i + by) % n) for i in range(n)])


def swap(x, axis, bit):
    n = lax.axis_size(axis)
    return lax.ppermute(x, axis, [(i, i ^ bit) for i in range(n)])


def spread(x, axes):
    copies = jnp.broadcast_to(x, (lax.axis_size(axes), *x.shape))
    return lax.all_to_all(copies, axes, 0, 0, tiled=True)


def ordered(mine, other, bit, axis):
    low = bit == 0
    return jnp.stack([jnp.where(low, mine, other), jnp.where(low, other, mine)], axis)


def pick(x, index, axis):
    return lax.dynamic_index_in_dim(x, index, axis, keepdims=False)


def dot(a, b):
    return jnp.dot(a, b, precision=HIGH, preferred_element_type=jnp.float32)


def gathered_column(panel):
    c = lax.axis_index("c")
    zh = lax.axis_index("zh")
    share, width = panel.shape
    part = width // 4

    def columns(which):
        first = which * part
        cuts = [lax.dynamic_slice_in_dim(panel, first + j * 2 * part, part, 1) for j in range(2)]
        return jnp.concatenate(cuts, axis=1)

    near = ordered(columns(c), swap(columns(1 - c), "c", 1), c, 0)
    near = near.reshape(2 * share, width // 2)
    far = swap(near, "zh", 1)
    both = jnp.concatenate([jnp.broadcast_to(r, (4, *r.shape)) for r in (near, far)], axis=1)
    both = lax.all_to_all(both, "y", 0, 0, tiled=True).reshape(4, 2, *near.shape)
    low = zh == 0
    return jnp.stack([jnp.where(low, both[:, 0], both[:, 1]), jnp.where(low, both[:, 1], both[:, 0])])


def gathered_over_zl(rows):
    zl = lax.axis_index("zl")
    rows = rows[None]
    for bit in (4, 2, 1):
        other = swap(rows, "zl", bit)
        rows = ordered(rows, other, zl & bit, 1 if bit != 4 else 0)
        rows = rows.reshape(-1, *rows.shape[2:])
    return rows


def reduced_over_zl(t):
    zl = lax.axis_index("zl")
    low, mid, high = zl % 2, (zl // 2) % 2, zl // 4
    t = pick(t, low, 3) + swap(pick(t, 1 - low, 3), "zl", 1)

    def part(flip_high, flip_mid):
        first = (0, high ^ flip_high, mid ^ flip_mid, 0, 0)
        return lax.dynamic_slice(t, first, (2, 1, 1, *t.shape[3:]))[:, 0, 0]

    got = []
    for flips in ((0, 1), (1, 0), (1, 1)):
        bit = flips[0] * 4 + flips[1] * 2
        got.append(swap(part(*flips), "zl", bit))
    return part(0, 0) + got[0] + got[1] + got[2]


def reduced_products(inverse_tiles, codes, column):
    x = lax.axis_index("x")
    block = inverse_tiles.shape[1]
    column = column.reshape(block, -1)
    first, second = inverse_tiles
    tiles = [
        jnp.where(codes[0] == i, first, jnp.where(codes[1] == i, second, 0.0)) for i in range(2)
    ]
    tiles = lax.optimization_barrier(jnp.stack(tiles))
    tiles = (tiles, swap(tiles, "c", 1))
    left = {}
    for r in range(2):
        rows = tiles[r].reshape(2, 4, 4, block // 16, block)
        rows = [pick(rows, (x + d) % 4, 2).reshape(block // 2, block) for d in range(4)]
        for d, cut in enumerate(lax.optimization_barrier(rows)):
            left[d, r] = cut

    def product(d, r):
        return dot(left[d, r], column)

    up_a = shift(product(2, 0), "x", 1)
    down_a = shift(product(2, 1), "x", -1)
    up_b = shift(product(1, 1), "x", 1)
    down_b = shift(product(3, 0), "x", -1)
    rest = lax.optimization_barrier([product(1, 0), product(3, 1)])
    up_c = shift(rest[0] + up_a, "x", 1)
    down_c = shift(rest[1] + down_a, "x", -1)
    return product(0, 0) + down_b + up_c, product(0, 1) + up_b + down_c


def local(inverse_tiles, tile_rows, panel, pivot_base):
    share, width = panel.shape
    block = inverse_tiles.shape[1]
    half = block // 2
    c = lax.axis_index("c")
    codes = tile_rows[:, 0]
    column = gathered_column(panel)
    u = gathered_over_zl(panel).reshape(8 * share, width).T
    u = u.reshape(2, 4, 4, 4, 8, 8 * share).transpose(0, 3, 2, 1, 4, 5)
    u = lax.optimization_barrier(u.reshape(2, block, 8 * share))
    other_u = swap(u, "c", 1)
    t = reduced_products(inverse_tiles, codes, column)
    trailing = reduced_over_zl(jnp.stack(t).reshape(2, 2, 2, 2, share, block))
    other = swap(trailing[1], "c", 1)
    low, high = ordered(trailing[0], other, c, 0)
    trailing = [x[:, j * half : (j + 1) * half] for j in range(2) for x in (low, high)]
    trailing = jnp.concatenate(trailing, axis=1)

    parts = [[t[r][:, j * half : (j + 1) * half] for j in range(2)] for r in range(2)]
    own = lax.optimization_barrier([dot(u[j], parts[0][j]) for j in range(2)])
    w = [own[j] + dot(other_u[j], parts[1][j]) for j in range(2)]
    w = jnp.concatenate([x.reshape(16, 4, 8, half) for x in w], axis=1)
    w = lax.all_to_all(w, ("y", "x"), 0, 0, tiled=True).sum(axis=0)
    w = jnp.concatenate([w, w])
    w = lax.all_to_all(w, ("zh", "zl"), 0, 0, tiled=True).sum(axis=0)
    w = spread(w, ("y", "c"))
    w = w.reshape(4, 2, 8, half).transpose(0, 2, 1, 3).reshape(share, block)
    return (-trailing, pivot_base + w)


def solution(mesh):
    finer = Mesh(mesh.devices.reshape(2, 4, 2, 8, 4), PROW + PCOL)
    placed = (P(PROW, PCOL, None), P(PROW, PCOL), P(PROW + PCOL, None), P(PCOL, None))

    return jax.shard_map(
        local,
        mesh=finer,
        in_specs=placed,
        out_specs=(P(PROW + PCOL, None), P(PCOL, None)),
        check_vma=False,
    )
```
